32 devices in a mesh: groups: 2 (over y), expert: 16 (over z, x, core), tensor: 1.
Axes of the slice: x: 2, y: 2, z: 4, core: 2. Of those that a mesh axis runs over, the one named last changes fastest.
Arguments:
- tokens: bfloat16 [64, 4096], P(('groups', 'expert')), parts along dimension 0, may hold values from -6 to 6
- expert_ids: int32 [64, 2], P(('groups', 'expert')), parts along dimension 0, may hold values from 0 to 3, all different within a row; in each aligned block of 2 rows (0 to 1, 2 to 3, ...) at most 2 rows name the same one
- gate_weights: float32 [64, 2], P(('groups', 'expert')), parts along dimension 0, may hold values from 0.2 to 1
- doc_ids: int32 [64], P(('groups', 'expert')), parts along dimension 0, may hold values from 0 to 3, never falling along the last dimension, each value on 1 to 16 neighbouring positions
- w_gate: bfloat16 [4096, 2048], P(None, ('expert', 'tensor')), may hold values from -0.09375 to 0.09375
- w_up: bfloat16 [4096, 2048], P(None, ('expert', 'tensor')), may hold values from -0.09375 to 0.09375
- w_down: bfloat16 [2048, 4096], P(('expert', 'tensor')), may hold values from -0.25 to 0.25
- w_score: float32 [4096], P('tensor'), may hold values from -0.375 to 0.375
Outputs:
- mixed: bfloat16 [64, 4096], P(('groups', 'expert'), 'tensor'), parts along dimension 0
- scores: float32 [8], P('groups'), parts along dimension 0
The draws below stay inside these ranges and needn't reach their ends.
There are 2 independent parts, one for each index of `groups`. The reference program is written for one: setup_inputs(seed, part) draws one part's arguments, and reference() takes and returns one part's arrays. A program takes and returns all parts, laid end to end along the dimension named above; an argument that names none is the same for every part. Nothing has to cross between parts.
Inputs may be any that keep to these rules, and one draw needn't show every extreme that they name: `expert_ids`: each row names two different experts. Among the rows of one device no expert is named more than 2 times, and in some devices' rows some expert exactly 2 times. `doc_ids`: document ids never fall along the tokens; every document holds 1 to 16 tokens, one exactly 16.
All inputs are finite; a program needn't handle non-finite values.
Results may differ from the reference program's by a relative error of at most 0.0057.
Values may be sent and summed in bfloat16 or wider, within the bound.
A program may use at most 64 MiB of HBM per device.

```python
import math
import jax
import jax.numpy as jnp
import numpy as np
from jax import lax

D = 4096
H_DEV = 128
EXP_FLIGHT = 4
TOK_DEV = 2
CAP = 2
TOKENS = 32
DOCS = 4
DOC_MOST = 16
FF_WIN = 512


def shard_levels(rng, shape, cuts, low, high):
    factor_of = 1.0
    for axis_at, shards_of in cuts:
        draws = jax.random.uniform(jax.random.fold_in(jax.random.fold_in(rng, 6), axis_at), (shards_of,), jnp.float32, low / len(cuts), high / len(cuts))
        factor_of = factor_of * jnp.repeat(jnp.exp(draws), shape[axis_at] // shards_of).reshape((-1,) + (1,) * (len(shape) - 1 - axis_at))
    return factor_of


def length_profile(number_of, total, limit, skew):
    loads = [(1 << 20) // math.isqrt(grade ** skew) + 1 for grade in range(2, number_of + 1)]
    rest, given = total - limit - (number_of - 1), [1] * (number_of - 1)
    while rest > 0:
        candidates = [i for i in range(number_of - 1) if given[i] < limit]
        mass, budget = sum([loads[i] for i in candidates]), rest
        for i in candidates:
            extra = min(limit - given[i], max(1, budget * loads[i] // mass), rest)
            given[i] = given[i] + extra
            rest = rest - extra
    return np.array([limit] + given)


def ragged_sizes(stream_key, number_of, total, limit, skew):
    if number_of == 2:
        one = jax.random.randint(stream_key, (), max(1, total - limit), min(limit, total - 1) + 1)
        return jnp.stack([one, total - one])
    tallies = jnp.asarray(length_profile(number_of, total, limit, skew), jnp.int32)
    twos = (number_of - 1) // 2
    giver, sink = tallies[1:1 + 2 * twos:2], tallies[2:2 + 2 * twos:2]
    room = jnp.minimum(giver - 1, limit - sink)
    moved = jax.random.randint(jax.random.fold_in(stream_key, 1), (twos,), 0, 1 << 20) % (room + 1)
    tallies = tallies.at[1:1 + 2 * twos:2].set(giver - moved).at[2:2 + 2 * twos:2].set(sink + moved)
    return tallies[jax.random.permutation(jax.random.fold_in(stream_key, 2), number_of)]


def routed_block(key, own, number, rows, amount, top, limit, lean):
    sequence = jax.random.permutation(key, amount)
    packed, ordinary = shares(amount, rows * top, limit, lean, True), shares(amount, rows * top, limit, lean, False)
    places = jnp.arange(amount)

    def named(sizes, rotation):
        used = int((sizes > 0).sum())
        fixed = max(1, used // 4)
        moved = fixed + (places - fixed + rotation * (used - fixed)) % max(1, amount - fixed)
        return jnp.zeros((amount,), jnp.int32).at[sequence[jnp.where(places < fixed, places, moved)]].set(jnp.asarray(sizes, jnp.int32))

    sizes = jnp.where(number % 4 == 0, named(packed, number // 4), named(ordinary, number - number // 4 - 1))
    mixed = jax.random.permutation(jax.random.fold_in(own, 3), amount)
    source_of, taker = mixed[0:amount // 2 * 2:2], mixed[1:amount // 2 * 2:2]
    room = jnp.minimum(sizes[source_of] - 1, limit - sizes[taker]) // 2
    room = jnp.where((source_of == sequence[0]) | (taker == sequence[0]) | (sizes[taker] == 0), 0, jnp.maximum(room, 0))
    moved = jax.random.randint(jax.random.fold_in(own, 4), (amount // 2,), 0, 1 << 20) % (room + 1)
    sizes = sizes.at[source_of].add(-moved).at[taker].add(moved)
    labels = jnp.searchsorted(jnp.cumsum(sizes), jnp.arange(rows * top), side="right").astype(jnp.int32)
    table = labels.reshape(top, rows).T
    table = table[jax.random.permutation(jax.random.fold_in(own, 1), rows)]
    rotation = jax.random.randint(jax.random.fold_in(own, 2), (rows, 1), 0, top)
    return jnp.take_along_axis(table, (jnp.arange(top)[None, :] + rotation) % top, axis=1)


def shares(amount, total, most, skew, full):
    weights = [(1 << 20) // math.isqrt(grade ** skew) + 1 for grade in range(1, amount + 1)]
    largest = most if full else min(most, max(-(-total // amount), total * weights[0] // sum(weights)))
    least = 1 if total - largest >= amount - 1 else 0
    given, spare = [largest] + [least] * (amount - 1), total - largest - least * (amount - 1)
    while spare > 0:
        candidates = [i for i in range(1, amount) if given[i] < largest] or [i for i in range(1, amount) if given[i] < most]
        pool, budget = sum([weights[i] for i in candidates]), spare
        for i in candidates:
            extra = min(most - given[i], max(1, budget * weights[i] // pool), spare)
            given[i] = given[i] + extra
            spare = spare - extra
    return np.array(given)


def scatter_about(own_key, dims, scale, bound, pieces=(), held_as=jnp.bfloat16):
    result = jax.random.normal(own_key, dims, jnp.float32) * scale
    if len(pieces) > 0:
        result = shard_levels(own_key, dims, pieces, -0.22, 0.18) * result
    return jnp.clip(result, min=-bound, max=bound).astype(held_as)


def setup_inputs(seed: int = 0, part: int = 0) -> dict:
    arg_keys = jax.random.split(jax.random.key(seed), 9)
    part_keys = jax.random.split(jax.random.fold_in(arg_keys[8], part), 9)
    tokens = scatter_about(part_keys[0], (TOKENS, D), 1.0, 6.0, ((0, 16),))
    expert_ids_keys = jax.random.split(jax.random.fold_in(part_keys[1], 1), TOKENS // TOK_DEV)
    expert_ids_turns = jax.random.permutation(jax.random.fold_in(part_keys[1], 3), TOKENS // TOK_DEV)
    expert_ids = jax.vmap(lambda own, number: routed_block(jax.random.fold_in(part_keys[1], 2), own, number, TOK_DEV, EXP_FLIGHT, 2, CAP, 1))(expert_ids_keys, expert_ids_turns).reshape((TOKENS, 2))
    gate_weights = jnp.clip(jnp.exp(math.log(1.0) - 1.609438 * jax.random.uniform(part_keys[2], (TOKENS, 2), jnp.float32) ** shard_levels(part_keys[2], (TOKENS, 2), ((0, 16),), -0.2, 0.2)), 0.2, 1.0)
    doc_ids = jnp.searchsorted(jnp.cumsum(ragged_sizes(part_keys[3], DOCS, TOKENS, DOC_MOST, 1)), jnp.arange(TOKENS), side="right").astype(jnp.int32)
    w_gate = scatter_about(arg_keys[4], (D, EXP_FLIGHT * FF_WIN), D ** -0.5, 0.09375, ((1, 16),))
    w_up = scatter_about(arg_keys[5], (D, EXP_FLIGHT * FF_WIN), D ** -0.5, 0.09375, ((1, 16),))
    w_down = scatter_about(arg_keys[6], (EXP_FLIGHT * FF_WIN, D), FF_WIN ** -0.5, 0.25, ((0, 16),))
    w_score = scatter_about(arg_keys[7], (D,), (4.0 / D ** 0.5), 0.375, (), jnp.float32)
    return dict(tokens=tokens, expert_ids=expert_ids, gate_weights=gate_weights, doc_ids=doc_ids, w_gate=w_gate, w_up=w_up, w_down=w_down, w_score=w_score)


def reference(tokens, expert_ids, gate_weights, doc_ids, w_gate, w_up, w_down, w_score):
    width = tokens.shape[1]
    nblocks = FF_WIN // H_DEV
    mixed_acc = jnp.zeros((TOKENS, width), jnp.float32)
    for expert in range(EXP_FLIGHT):
        first = expert * FF_WIN
        gate_part = jnp.dot(tokens, w_gate[:, first:first + FF_WIN], preferred_element_type=jnp.float32)
        up_part = jnp.dot(tokens, w_up[:, first:first + FF_WIN], preferred_element_type=jnp.float32)
        hidden = (jax.nn.silu(gate_part) * up_part).astype(jnp.bfloat16)
        hidden_blocks = hidden.reshape(TOKENS, nblocks, H_DEV).transpose(1, 0, 2)
        down_blocks = w_down[first:first + FF_WIN].reshape(nblocks, H_DEV, width)

        def add_block(total, pair):
            piece = jnp.dot(pair[0], pair[1], preferred_element_type=jnp.float32).astype(jnp.bfloat16)
            piece = lax.optimization_barrier(piece)
            return total + piece.astype(jnp.float32), None

        expert_out, _ = lax.scan(add_block, jnp.zeros((TOKENS, width), jnp.float32), (hidden_blocks, down_blocks))
        weight = jnp.sum(jnp.where(expert_ids == expert, gate_weights, jnp.float32(0.0)), axis=1)
        mixed_acc = mixed_acc + weight[:, None] * expert_out
    mixed = mixed_acc.astype(jnp.bfloat16)
    projected = jnp.dot(mixed.astype(jnp.float32), w_score, precision=lax.Precision.HIGHEST)
    docs_hit = (doc_ids[:, None] == jnp.arange(DOCS, dtype=jnp.int32)[None, :]).astype(jnp.float32)
    totals = jnp.dot(projected, docs_hit, precision=lax.Precision.HIGHEST)
    counts = jnp.sum(docs_hit, axis=0)
    scores = jax.nn.sigmoid(totals / counts)
    return mixed, scores
```

```python
import functools

import jax
import jax.numpy as jnp
from jax import lax
from jax.experimental import pallas as pl
from jax.experimental.pallas import tpu as pltpu
from jax.sharding import PartitionSpec as P

EXP_FLIGHT = 4
LANES = 128
DOC_LANE = 64
MESH = pl.DeviceIdType.MESH
F32 = jnp.float32
BF16 = jnp.bfloat16


def is_pow2(n):
    return n & (n - 1) == 0


def partner(x, m, n):
    if not is_pow2(n):
        return lax.rem(x + m, n)
    out, bit = x, 1
    while bit < n:
        if m & bit:
            out = out + bit - 2 * bit * lax.rem(lax.div(x, bit), 2)
        bit *= 2
    return out


def source(x, m, n):
    return partner(x, m, n) if is_pow2(n) else lax.rem(x + n - m, n)


def three_parts(x):
    hi = x.astype(BF16).astype(F32)
    rest = x - hi
    mid = rest.astype(BF16).astype(F32)
    low = (rest - mid).astype(BF16).astype(F32)
    return hi, mid, low


def kernel(
    A, B, T, C, docs,
    tok_hbm, ids_hbm, gw_hbm, doc_hbm, wg_hbm, wu_hbm, wd_hbm, ws_hbm,
    mixed_ref, scores_ref,
    gathered, w1, w2, ws, ids, gw, doc,
    send1, recv1, send2, recv2, sums1, got1, sums2, got2,
    load_sem, z_send, z_recv, p_send, p_recv, r1_send, r1_recv, r2_send, r2_recv,
    s1_send, s1_recv, s2_send, s2_recv,
):
    rows, D = tok_hbm.shape
    hid = wg_hbm.shape[1]
    DT = D // T
    DC = DT // C
    Q = B * T
    me = lax.axis_index("expert")
    j = lax.axis_index("tensor")
    a, b = lax.div(me, B), lax.rem(me, B)
    q = b * T + j

    def z_peer(m):
        return {"expert": partner(a, m, A) * B + b, "tensor": j}

    def p_peer(m):
        return {"expert": a * B + partner(b, m, B), "tensor": j}

    def q_peer(m):
        to = partner(q, m, Q)
        return {"expert": a * B + lax.div(to, T), "tensor": lax.rem(to, T)}

    own = b * A + a
    loads = [
        pltpu.make_async_copy(tok_hbm, gathered.at[own, :, pl.ds(0, D)], load_sem.at[0]),
        pltpu.make_async_copy(ids_hbm, ids, load_sem.at[1]),
        pltpu.make_async_copy(gw_hbm, gw, load_sem.at[2]),
        pltpu.make_async_copy(doc_hbm, doc, load_sem.at[3]),
        pltpu.make_async_copy(wg_hbm, w1.at[:, pl.ds(0, hid)], load_sem.at[4]),
        pltpu.make_async_copy(wu_hbm, w1.at[:, pl.ds(hid, hid)], load_sem.at[5]),
        pltpu.make_async_copy(wd_hbm, w2, load_sem.at[6]),
        pltpu.make_async_copy(ws_hbm, ws, load_sem.at[7]),
    ]
    barrier = pltpu.get_barrier_semaphore()
    for m in range(1, A):
        pl.semaphore_signal(barrier, inc=1, device_id=z_peer(m), device_id_type=MESH)
    for m in range(1, Q):
        pl.semaphore_signal(barrier, inc=1, device_id=q_peer(m), device_id_type=MESH)
    for copy in loads:
        copy.start()

    for copy in loads[1:4]:
        copy.wait()
    lane = lax.broadcasted_iota(jnp.int32, (rows, LANES), 1)
    row = lax.broadcasted_iota(jnp.int32, (rows, LANES), 0)
    meta = jnp.zeros((rows, LANES), F32)
    for r in range(rows):
        for k in range(2):
            chosen, weight = ids[r, k], gw[r, k]
            for part, value in enumerate(three_parts(jnp.full((rows, LANES), weight, F32))):
                meta = jnp.where((row == r) & (lane == part * A + chosen), value, meta)
        meta = jnp.where((row == r) & (lane == DOC_LANE + doc[r]), F32(1.0), meta)
    gathered[own, :, pl.ds(D, LANES)] = meta.astype(BF16)
    loads[0].wait()
    pl.semaphore_wait(barrier, (A - 1) + (Q - 1))

    zs = {}
    for m in reversed(range(1, A)):
        zs[m] = pltpu.make_async_remote_copy(
            src_ref=gathered.at[own], dst_ref=gathered.at[own],
            send_sem=z_send.at[m - 1], recv_sem=z_recv.at[m - 1],
            device_id=z_peer(m), device_id_type=MESH,
        )
        zs[m].start()
    ps = []

    def forward(step):
        slot = b * A + source(a, step, A)
        for m in reversed(range(1, B)):
            at = step * (B - 1) + m - 1
            copy = pltpu.make_async_remote_copy(
                src_ref=gathered.at[slot], dst_ref=gathered.at[slot],
                send_sem=p_send.at[at], recv_sem=p_recv.at[at],
                device_id=p_peer(m), device_id_type=MESH,
            )
            copy.start()
            ps.append(copy)

    forward(0)
    loads[6].wait()
    loads[7].wait()
    hi, mid, low = three_parts(ws[...])
    srow = lax.broadcasted_iota(jnp.int32, (16, D), 0)
    left = jnp.where(srow == 0, hi, jnp.where(srow == 1, mid, jnp.where(srow == 2, low, 0.0)))
    seen = lax.dot_general(
        left.astype(BF16), w2[...], (((1,), (1,)), ((), ())), preferred_element_type=F32
    )
    seen = jnp.sum(seen, axis=0, keepdims=True)
    loads[4].wait()
    loads[5].wait()
    for m in range(1, A):
        zs[m].wait_recv()
        forward(m)
    for copy in ps:
        copy.wait_recv()

    n_tok = A * B * rows
    everyone = gathered[...].reshape(n_tok, D + LANES)
    x = everyone[:, :D]
    meta = everyone[:, D:].astype(F32)
    lane = lax.broadcasted_iota(jnp.int32, (n_tok, LANES), 1)
    mine = (lane < 3 * A) & (lax.rem(lane, A) == a)
    weight = jnp.sum(jnp.where(mine, meta, 0.0), axis=1, keepdims=True)
    hits = jnp.where(lane >= DOC_LANE, meta, 0.0)
    both = jnp.dot(x, w1[...], preferred_element_type=F32)
    gate, up = both[:, :hid], both[:, hid:]
    hidden = ((gate / (1.0 + jnp.exp(-gate))) * up).astype(BF16)

    firsts = []
    for c in range(C):
        for t in range(T):
            part = jnp.dot(
                hidden, w2[:, t * DT + c * DC:t * DT + (c + 1) * DC], preferred_element_type=F32
            )
            part = (part * weight).reshape(B, A * rows, DC)
            send1[t, :, :, c * DC:(c + 1) * DC] = part.astype(BF16)
        for m in reversed(range(1, Q)):
            to = partner(q, m, Q)
            at = c * (Q - 1) + m - 1
            copy = pltpu.make_async_remote_copy(
                src_ref=send1.at[lax.rem(to, T), lax.div(to, T), :, pl.ds(c * DC, DC)],
                dst_ref=recv1.at[m - 1, :, pl.ds(c * DC, DC)],
                send_sem=r1_send.at[at], recv_sem=r1_recv.at[at],
                device_id=q_peer(m), device_id_type=MESH,
            )
            copy.start()
            firsts.append((c, copy))
    seen_by = jnp.sum(hidden.astype(F32) * seen, axis=1, keepdims=True) * weight
    sums = jnp.sum(hits * seen_by, axis=0, keepdims=True)
    counts = jnp.sum(hits, axis=0, keepdims=True)
    sums1[...] = jnp.broadcast_to(sums, (8, LANES))
    s_first = []
    for m in range(1, Q):
        copy = pltpu.make_async_remote_copy(
            src_ref=sums1, dst_ref=got1.at[m - 1],
            send_sem=s1_send.at[m - 1], recv_sem=s1_recv.at[m - 1],
            device_id=q_peer(m), device_id_type=MESH,
        )
        copy.start()
        s_first.append(copy)

    seconds = []
    for c in range(C):
        for at, copy in firsts:
            if at == c:
                copy.wait_recv()
        cols = pl.ds(c * DC, DC)
        total = send1[j, b, :, cols].astype(F32)
        for m in range(1, Q):
            total = total + recv1[m - 1, :, cols].astype(F32)
        for to in range(A):
            send2[to, :, cols] = total[to * rows:(to + 1) * rows].astype(BF16)
        for m in reversed(range(1, A)):
            at = c * (A - 1) + m - 1
            copy = pltpu.make_async_remote_copy(
                src_ref=send2.at[partner(a, m, A), :, cols],
                dst_ref=recv2.at[m - 1, :, cols],
                send_sem=r2_send.at[at], recv_sem=r2_recv.at[at],
                device_id=z_peer(m), device_id_type=MESH,
            )
            copy.start()
            seconds.append((c, copy))
    for copy in s_first:
        copy.wait_recv()
    plane = sums1[...]
    for m in range(1, Q):
        plane = plane + got1[m - 1]
    sums2[...] = plane
    s_second = []
    for m in reversed(range(1, A)):
        copy = pltpu.make_async_remote_copy(
            src_ref=sums2, dst_ref=got2.at[m - 1],
            send_sem=s2_send.at[m - 1], recv_sem=s2_recv.at[m - 1],
            device_id=z_peer(m), device_id_type=MESH,
        )
        copy.start()
        s_second.append(copy)

    for c in range(C):
        for at, copy in seconds:
            if at == c:
                copy.wait_recv()
        cols = pl.ds(c * DC, DC)
        total = send2[a, :, cols].astype(F32)
        for m in range(1, A):
            total = total + recv2[m - 1, :, cols].astype(F32)
        mixed_ref[:, cols] = total.astype(BF16)
    for copy in s_second:
        copy.wait_recv()
    totals = sums2[...]
    for m in range(1, A):
        totals = totals + got2[m - 1]
    mean = totals[0:1, DOC_LANE:DOC_LANE + docs] / counts[:, DOC_LANE:DOC_LANE + docs]
    scores_ref[...] = 1.0 / (1.0 + jnp.exp(-mean))

    for copy in list(zs.values()) + ps + [c for _, c in firsts] + s_first:
        copy.wait_send()
    for copy in [c for _, c in seconds] + s_second:
        copy.wait_send()


def solution(mesh):
    E, T = mesh.shape["expert"], mesh.shape["tensor"]
    A = EXP_FLIGHT
    B = E // A
    Q = B * T

    def local(tokens, expert_ids, gate_weights, doc_ids, w_gate, w_up, w_down, w_score):
        rows, D = tokens.shape
        hid = w_gate.shape[1]
        docs = rows * E // 8
        assert 3 * A <= DOC_LANE and DOC_LANE + docs <= LANES
        DT = D // T
        C = next(c for c in (4, 2, 1) if DT % (c * LANES) == 0)
        if T > 1:
            w_score = lax.all_gather(w_score, "tensor", tiled=True)
        dma = pltpu.SemaphoreType.DMA
        any_spec = pl.BlockSpec(memory_space=pl.ANY)
        mixed, scores = pl.pallas_call(
            functools.partial(kernel, A, B, T, C, docs),
            out_shape=(
                jax.ShapeDtypeStruct((rows, DT), BF16),
                jax.ShapeDtypeStruct((1, docs), F32),
            ),
            in_specs=[any_spec] * 8,
            out_specs=(
                pl.BlockSpec(memory_space=pltpu.VMEM),
                pl.BlockSpec(memory_space=pltpu.VMEM),
            ),
            scratch_shapes=[
                pltpu.VMEM((E, rows, D + LANES), BF16),
                pltpu.VMEM((D, 2 * hid), BF16),
                pltpu.VMEM((hid, D), BF16),
                pltpu.VMEM((1, D), F32),
                pltpu.SMEM(expert_ids.shape, jnp.int32),
                pltpu.SMEM(gate_weights.shape, F32),
                pltpu.SMEM(doc_ids.shape, jnp.int32),
                pltpu.VMEM((T, B, A * rows, DT), BF16),
                pltpu.VMEM((Q - 1, A * rows, DT), BF16),
                pltpu.VMEM((A, rows, DT), BF16),
                pltpu.VMEM((A - 1, rows, DT), BF16),
                pltpu.VMEM((8, LANES), F32),
                pltpu.VMEM((Q - 1, 8, LANES), F32),
                pltpu.VMEM((8, LANES), F32),
                pltpu.VMEM((A - 1, 8, LANES), F32),
                dma((8,)),
                dma((A - 1,)), dma((A - 1,)),
                dma((A * (B - 1),)), dma((A * (B - 1),)),
                dma((C * (Q - 1),)), dma((C * (Q - 1),)),
                dma((C * (A - 1),)), dma((C * (A - 1),)),
                dma((Q - 1,)), dma((Q - 1,)),
                dma((A - 1,)), dma((A - 1,)),
            ],
            compiler_params=pltpu.CompilerParams(collective_id=0, has_side_effects=True),
        )(
            tokens, expert_ids, gate_weights, doc_ids, w_gate, w_up, w_down,
            w_score.reshape(1, D),
        )
        return mixed, scores.reshape(docs)

    in_specs = (
        P(("groups", "expert"), None),
        P(("groups", "expert"), None),
        P(("groups", "expert"), None),
        P(("groups", "expert")),
        P(None, ("expert", "tensor")),
        P(None, ("expert", "tensor")),
        P(("expert", "tensor"), None),
        P("tensor"),
    )
    out_specs = (P(("groups", "expert"), "tensor"), P("groups"))
    return jax.shard_map(local, mesh=mesh, in_specs=in_specs, out_specs=out_specs, check_vma=False)
```

```python
import functools

import jax
import jax.numpy as jnp
from jax import lax
from jax.experimental import pallas as pl
from jax.experimental.pallas import tpu as pltpu
from jax.sharding import PartitionSpec as P

EXP_FLIGHT = 4
CORES = 2
CHUNKS = 2
LANES = 128
DOC_LANE = 64
MESH = pl.DeviceIdType.MESH
F32 = jnp.float32
BF16 = jnp.bfloat16


def is_pow2(n):
    return n & (n - 1) == 0


def partner(x, m, n):
    if not is_pow2(n):
        return lax.rem(x + m, n)
    out, bit = x, 1
    while bit < n:
        if m & bit:
            out = out + bit - 2 * bit * lax.rem(lax.div(x, bit), 2)
        bit *= 2
    return out


def source(x, m, n):
    return partner(x, m, n) if is_pow2(n) else lax.rem(x + n - m, n)


def three_parts(x):
    hi = x.astype(BF16).astype(F32)
    rest = x - hi
    mid = rest.astype(BF16).astype(F32)
    low = (rest - mid).astype(BF16).astype(F32)
    return hi, mid, low


def kernel(
    spread, L, T, C, docs,
    tok_hbm, ids_hbm, gw_hbm, doc_hbm, wg_hbm, wu_hbm, wd_hbm, ws_hbm,
    mixed_ref, scores_ref,
    gathered, w1, w2, ws, ids, gw, doc,
    send1, recv1, kept, send2, recv2, sums1, got1, sums2, got2,
    load_sem, g_send, g_recv, p_send, p_recv, r1_send, r1_recv, r2_send, r2_recv,
    s1_send, s1_recv, s2_send, s2_recv,
):
    rows, D = tok_hbm.shape
    hid = wg_hbm.shape[1]
    DT = D // T
    DC = DT // C
    A = EXP_FLIGHT
    slots = gathered.shape[0]
    me = lax.axis_index("expert")
    j = lax.axis_index("tensor")
    flat = me * T + j
    core, chip = lax.rem(flat, CORES), lax.div(flat, CORES)
    expert = lax.div(me, spread)

    def device(core, chip):
        to = chip * CORES + core
        return {"expert": lax.div(to, T), "tensor": lax.rem(to, T)}

    def line_peer(m):
        return device(core, partner(chip, m, L))

    other_core = device(1 - core, chip)

    def slot_of(core, chip):
        return core * L + chip if T == 1 else chip

    own = slot_of(core, chip)
    loads = [
        pltpu.make_async_copy(tok_hbm, gathered.at[own, :, pl.ds(0, D)], load_sem.at[0]),
        pltpu.make_async_copy(ids_hbm, ids, load_sem.at[1]),
        pltpu.make_async_copy(gw_hbm, gw, load_sem.at[2]),
        pltpu.make_async_copy(doc_hbm, doc, load_sem.at[3]),
        pltpu.make_async_copy(wg_hbm, w1.at[:, pl.ds(0, hid)], load_sem.at[4]),
        pltpu.make_async_copy(wu_hbm, w1.at[:, pl.ds(hid, hid)], load_sem.at[5]),
        pltpu.make_async_copy(wd_hbm, w2, load_sem.at[6]),
        pltpu.make_async_copy(ws_hbm, ws, load_sem.at[7]),
    ]
    barrier = pltpu.get_barrier_semaphore()
    for m in reversed(range(1, L)):
        pl.semaphore_signal(barrier, inc=1, device_id=line_peer(m), device_id_type=MESH)
    pl.semaphore_signal(barrier, inc=1, device_id=other_core, device_id_type=MESH)
    for copy in loads:
        copy.start()

    for copy in loads[1:4]:
        copy.wait()
    lane = lax.broadcasted_iota(jnp.int32, (rows, LANES), 1)
    row = lax.broadcasted_iota(jnp.int32, (rows, LANES), 0)
    meta = jnp.zeros((rows, LANES), F32)
    for r in range(rows):
        for k in range(2):
            chosen, weight = ids[r, k], gw[r, k]
            for part, value in enumerate(three_parts(jnp.full((rows, LANES), weight, F32))):
                meta = jnp.where((row == r) & (lane == part * A + chosen), value, meta)
        meta = jnp.where((row == r) & (lane == DOC_LANE + doc[r]), F32(1.0), meta)
    gathered[own, :, pl.ds(D, LANES)] = meta.astype(BF16)
    loads[0].wait()
    pl.semaphore_wait(barrier, L)

    straight = {}
    for m in reversed(range(1, L)):
        straight[m] = pltpu.make_async_remote_copy(
            src_ref=gathered.at[own], dst_ref=gathered.at[own],
            send_sem=g_send.at[m - 1], recv_sem=g_recv.at[m - 1],
            device_id=line_peer(m), device_id_type=MESH,
        )
        straight[m].start()
    passed = []

    def forward(m):
        slot = slot_of(core, source(chip, m, L))
        copy = pltpu.make_async_remote_copy(
            src_ref=gathered.at[slot], dst_ref=gathered.at[slot],
            send_sem=p_send.at[m], recv_sem=p_recv.at[m],
            device_id=other_core, device_id_type=MESH,
        )
        copy.start()
        passed.append(copy)

    if T == 1:
        forward(0)
    loads[6].wait()
    loads[7].wait()
    hi, mid, low = three_parts(ws[...])
    srow = lax.broadcasted_iota(jnp.int32, (16, D), 0)
    left = jnp.where(srow == 0, hi, jnp.where(srow == 1, mid, jnp.where(srow == 2, low, 0.0)))
    seen = lax.dot_general(
        left.astype(BF16), w2[...], (((1,), (1,)), ((), ())), preferred_element_type=F32
    )
    seen = jnp.sum(seen, axis=0, keepdims=True)
    loads[4].wait()
    loads[5].wait()
    for m in range(1, L):
        straight[m].wait_recv()
        if T == 1:
            forward(m)
    for copy in passed:
        copy.wait_recv()

    n_tok = slots * rows
    everyone = gathered[...].reshape(n_tok, D + LANES)
    x = everyone[:, :D]
    meta = everyone[:, D:].astype(F32)
    lane = lax.broadcasted_iota(jnp.int32, (n_tok, LANES), 1)
    mine = (lane < 3 * A) & (lax.rem(lane, A) == expert)
    weight = jnp.sum(jnp.where(mine, meta, 0.0), axis=1, keepdims=True)
    hits = jnp.where(lane >= DOC_LANE, meta, 0.0)
    both = jnp.dot(x, w1[...], preferred_element_type=F32)
    gate, up = both[:, :hid], both[:, hid:]
    hidden = ((gate / (1.0 + jnp.exp(-gate))) * up).astype(BF16)

    firsts = []
    for c in range(C):
        if T == 1:
            part = jnp.dot(hidden, w2[:, c * DC:(c + 1) * DC], preferred_element_type=F32) * weight
            low_half, high_half = part[:L * rows], part[L * rows:]
        else:
            low_half, high_half = (
                jnp.dot(
                    hidden, w2[:, h * DT + c * DC:h * DT + (c + 1) * DC],
                    preferred_element_type=F32,
                ) * weight
                for h in range(CORES)
            )
        cols = pl.ds(c * DC, DC)
        send1[:, cols] = jnp.where(core == 0, high_half, low_half).astype(BF16)
        copy = pltpu.make_async_remote_copy(
            src_ref=send1.at[:, cols], dst_ref=recv1.at[:, cols],
            send_sem=r1_send.at[c], recv_sem=r1_recv.at[c],
            device_id=other_core, device_id_type=MESH,
        )
        copy.start()
        firsts.append(copy)
        kept[:, cols] = jnp.where(core == 0, low_half, high_half)
    seen_by = jnp.sum(hidden.astype(F32) * seen, axis=1, keepdims=True) * weight
    sums1[...] = jnp.sum(hits * seen_by, axis=0, keepdims=True)
    counts = jnp.sum(hits, axis=0, keepdims=True)
    s_first = pltpu.make_async_remote_copy(
        src_ref=sums1, dst_ref=got1, send_sem=s1_send.at[0], recv_sem=s1_recv.at[0],
        device_id=other_core, device_id_type=MESH,
    )
    s_first.start()

    seconds = []
    for c in range(C):
        firsts[c].wait_recv()
        cols = pl.ds(c * DC, DC)
        total = kept[:, cols] + recv1[:, cols].astype(F32)
        for to in range(L):
            send2[to, :, cols] = total[to * rows:(to + 1) * rows].astype(BF16)
        for m in reversed(range(1, L)):
            at = c * (L - 1) + m - 1
            copy = pltpu.make_async_remote_copy(
                src_ref=send2.at[partner(chip, m, L), :, cols],
                dst_ref=recv2.at[m - 1, :, cols],
                send_sem=r2_send.at[at], recv_sem=r2_recv.at[at],
                device_id=line_peer(m), device_id_type=MESH,
            )
            copy.start()
            seconds.append((c, copy))
        if c == 0:
            s_first.wait_recv()
            sums2[...] = sums1[...] + got1[...]
            s_second = []
            for m in reversed(range(1, L)):
                copy = pltpu.make_async_remote_copy(
                    src_ref=sums2, dst_ref=got2.at[m - 1],
                    send_sem=s2_send.at[m - 1], recv_sem=s2_recv.at[m - 1],
                    device_id=line_peer(m), device_id_type=MESH,
                )
                copy.start()
                s_second.append(copy)

    for copy in s_second:
        copy.wait_recv()
    totals = sums2[...]
    for m in range(1, L):
        totals = totals + got2[m - 1]
    docs_at = slice(DOC_LANE, DOC_LANE + docs)
    mean = totals[:, docs_at] / counts[:, docs_at]
    scores_ref[...] = 1.0 / (1.0 + jnp.exp(-mean))
    for c in range(C):
        for at, copy in seconds:
            if at == c:
                copy.wait_recv()
        cols = pl.ds(c * DC, DC)
        total = send2[chip, :, cols].astype(F32)
        for m in range(1, L):
            total = total + recv2[m - 1, :, cols].astype(F32)
        mixed_ref[:, cols] = total.astype(BF16)

    for copy in list(straight.values()) + passed + firsts + [s_first]:
        copy.wait_send()
    for copy in [c for _, c in seconds] + s_second:
        copy.wait_send()


def solution(mesh):
    E, T = mesh.shape["expert"], mesh.shape["tensor"]
    assert T in (1, CORES) and E * T % CORES == 0
    L = E * T // CORES

    def local(tokens, expert_ids, gate_weights, doc_ids, w_gate, w_up, w_down, w_score):
        rows, D = tokens.shape
        hid = w_gate.shape[1]
        docs = rows * E // 8
        assert 3 * EXP_FLIGHT <= DOC_LANE and DOC_LANE + docs <= LANES
        DT = D // T
        C = next(c for c in (CHUNKS, 1) if DT % (c * LANES) == 0)
        if T > 1:
            w_score = lax.all_gather(w_score, "tensor", tiled=True)
        dma = pltpu.SemaphoreType.DMA
        any_spec = pl.BlockSpec(memory_space=pl.ANY)
        mixed, scores = pl.pallas_call(
            functools.partial(kernel, E // EXP_FLIGHT, L, T, C, docs),
            out_shape=(
                pltpu.VMEM((rows, DT), BF16),
                pltpu.VMEM((1, docs), F32),
            ),
            in_specs=[any_spec] * 8,
            out_specs=(
                pl.BlockSpec(memory_space=pltpu.VMEM),
                pl.BlockSpec(memory_space=pltpu.VMEM),
            ),
            scratch_shapes=[
                pltpu.VMEM((E, rows, D + LANES), BF16),
                pltpu.VMEM((D, 2 * hid), BF16),
                pltpu.VMEM((hid, D), BF16),
                pltpu.VMEM((1, D), F32),
                pltpu.SMEM(expert_ids.shape, jnp.int32),
                pltpu.SMEM(gate_weights.shape, F32),
                pltpu.SMEM(doc_ids.shape, jnp.int32),
                pltpu.VMEM((L * rows, DT), BF16),
                pltpu.VMEM((L * rows, DT), BF16),
                pltpu.VMEM((L * rows, DT), F32),
                pltpu.VMEM((L, rows, DT), BF16),
                pltpu.VMEM((L - 1, rows, DT), BF16),
                pltpu.VMEM((1, LANES), F32),
                pltpu.VMEM((1, LANES), F32),
                pltpu.VMEM((1, LANES), F32),
                pltpu.VMEM((L - 1, 1, LANES), F32),
                dma((8,)),
                dma((L - 1,)), dma((L - 1,)),
                dma((L,)), dma((L,)),
                dma((C,)), dma((C,)),
                dma((C * (L - 1),)), dma((C * (L - 1),)),
                dma((1,)), dma((1,)),
                dma((L - 1,)), dma((L - 1,)),
            ],
            compiler_params=pltpu.CompilerParams(collective_id=0, has_side_effects=True),
        )(
            tokens, expert_ids, gate_weights, doc_ids, w_gate, w_up, w_down,
            w_score.reshape(1, D),
        )
        return mixed, scores.reshape(docs)

    in_specs = (
        P(("groups", "expert"), None),
        P(("groups", "expert"), None),
        P(("groups", "expert"), None),
        P(("groups", "expert")),
        P(None, ("expert", "tensor")),
        P(None, ("expert", "tensor")),
        P(("expert", "tensor"), None),
        P("tensor"),
    )
    out_specs = (P(("groups", "expert"), "tensor"), P("groups"))
    return jax.shard_map(local, mesh=mesh, in_specs=in_specs, out_specs=out_specs, check_vma=False)
```
